256 devices in a mesh: tile: 128 (over y, x, z), rhs: 2 (over core).
Axes of the slice: x: 4, y: 4, z: 8, core: 2. Of those that a mesh axis runs over, the one named last changes fastest.
Arguments:
- sensitivity: bfloat16 [131072, 5120], P('tile', 'rhs'), may hold values from -0.0625 to 0.0625
- precision: float32 [5120], P('rhs'), may hold values from 3 to 60
- reaction: float32 [1024, 128], P('tile'), may hold values from 0.25 to 2
- load: float32 [64, 131072], P(None, 'tile'), may hold values from -24 to 24
Outputs:
- solution: float32 [64, 131072], P(None, 'tile')
- residual: float32 [64, 131072], P(None, 'tile')
The draws below stay inside these ranges and needn't reach their ends.
All inputs are finite; a program needn't handle non-finite values.
Results may differ from the reference program's by a relative error of at most 0.0042.
Values may be sent and summed in bfloat16 or wider, within the bound.
No kernel may reach another device: no remote copies, remote signals or barrier semaphores. Data moves between devices by JAX's collectives and lax.ppermute only.
A program may use at most 64 MiB of HBM per device.

```python
import math
import jax
import jax.numpy as jnp
from jax import lax

GY = 128
RHS = 64
ITERS = 2
NX = 1024
PARAMS = 131072
OBS = 5120


def with_spikes(entries, key, source, target, blocks, factor):
    def block_of(dim):
        return (jnp.arange(entries.shape[dim]) // (entries.shape[dim] // blocks)).reshape((-1,) + (1,) * (entries.ndim - 1 - dim))

    first = jax.random.permutation(key, blocks)[block_of(target)]
    other_side = (block_of(target) + blocks // 2) % blocks
    return jnp.where((block_of(source) == first) | (block_of(source) == other_side), factor * entries, entries)


def shard_levels(own_key, shape, split, smallest, top_value):
    factor_of, own = 1.0, jax.random.fold_in(own_key, 6)
    for dim, blocks in split:
        steps = jnp.exp(jax.random.uniform(jax.random.fold_in(own, dim), (blocks,), jnp.float32, smallest / len(split), top_value / len(split)))
        factor_of = factor_of * jnp.repeat(steps, shape[dim] // blocks).reshape([-1 if axis == dim else 1 for axis in range(len(shape))])
    return factor_of


def noise(stream_key, shape, deviation, most, split=(), kind=jnp.bfloat16):
    drawn = deviation * jax.random.normal(stream_key, shape, jnp.float32)
    if split:
        drawn = drawn * shard_levels(stream_key, shape, split, -0.22, 0.18)
    return jnp.clip(drawn, -most, most).astype(kind)


def noise_with(rng, shape, scale, bound, shards, heavy, held_as=jnp.bfloat16):
    values = scale * jax.random.normal(rng, shape, jnp.float32)
    if shards:
        values = values * shard_levels(rng, shape, shards, -0.22, 0.18)
    return jnp.clip(with_spikes(values, jax.random.fold_in(rng, 3), *heavy), -bound, bound).astype(held_as)


def setup_inputs(seed: int = 0) -> dict:
    arg_keys = jax.random.split(jax.random.key(seed), 5)
    sensitivity = noise_with(arg_keys[0], (PARAMS, OBS), PARAMS ** -0.5, 0.0625, ((0, 128), (1, 2)), (0, 1, 128, 5.5))
    precision = jnp.clip(jnp.exp(math.log(60.0) - 2.9957323 * jax.random.uniform(arg_keys[1], (OBS,), jnp.float32) ** shard_levels(arg_keys[1], (OBS,), ((0, 2),), -0.2, 0.2)), 3.0, 60.0)
    reaction = jnp.clip(jnp.exp(math.log(2.0) - 2.0794415 * jax.random.uniform(arg_keys[2], (NX, GY), jnp.float32) ** shard_levels(arg_keys[2], (NX, GY), ((0, 128),), -0.2, 0.2)), 0.25, 2.0)
    load = noise(arg_keys[3], (RHS, PARAMS), 4.0, 24.0, ((1, 128),), jnp.float32)
    return {"sensitivity": sensitivity, "precision": precision, "reaction": reaction, "load": load}


def apply_stencil(field, reaction):
    padded = jnp.pad(field, ((0, 0), (1, 1), (1, 1)))
    neighbours = padded[:, 2:, 1:-1] + padded[:, :-2, 1:-1] + padded[:, 1:-1, 2:] + padded[:, 1:-1, :-2]
    return (reaction + 4.0) * field - neighbours


def hessian(direction, sensitivity, precision, reaction):
    lowered = direction.astype(jnp.bfloat16)
    predicted = jnp.dot(lowered, sensitivity, preferred_element_type=jnp.float32)
    weighted = (precision[None, :] * predicted).astype(jnp.bfloat16)
    back = lax.dot_general(weighted, sensitivity, (((1,), (1,)), ((), ())), preferred_element_type=jnp.float32)
    grid = direction.reshape(direction.shape[0], reaction.shape[0], reaction.shape[1])
    twice = apply_stencil(apply_stencil(grid, reaction), reaction)
    return back + twice.reshape(direction.shape)


def reference(sensitivity, precision, reaction, load):
    solution = jnp.zeros_like(load)
    residual = load
    direction = load
    current = jnp.sum(residual * residual, axis=1)
    for iteration in range(ITERS):
        image = hessian(direction, sensitivity, precision, reaction)
        alpha = current / jnp.sum(direction * image, axis=1)
        solution = solution + alpha[:, None] * direction
        residual = residual - alpha[:, None] * image
        if iteration + 1 < ITERS:
            fresh = jnp.sum(residual * residual, axis=1)
            direction = residual + (fresh / current)[:, None] * direction
            current = fresh
    return solution, residual
```

```python
import jax
import jax.numpy as jnp
from jax import lax
from jax.sharding import Mesh
from jax.sharding import PartitionSpec as P

TILE = ("tile_0", "tile_1", "tile_2")
SWAP = [(0, 1), (1, 0)]
F32, BF16 = jnp.float32, jnp.bfloat16


def split3(x):
    hi = lax.reduce_precision(x, 8, 7)
    mid = lax.reduce_precision(x - hi, 8, 7)
    low = x - hi - mid
    return jnp.stack([hi, mid, low], axis=-1).astype(BF16)


def with_halo(block, dim, width):
    count = lax.axis_size(TILE)
    forward = [(i, i + 1) for i in range(count - 1)]
    backward = [(i + 1, i) for i in range(count - 1)]
    size = block.shape[dim]
    low = lax.ppermute(lax.slice_in_dim(block, size - width, size, axis=dim), TILE, forward)
    high = lax.ppermute(lax.slice_in_dim(block, 0, width, axis=dim), TILE, backward)
    return jnp.concatenate([low, block, high], axis=dim)


def stencil_rows(padded_field, reaction):
    sided = jnp.pad(padded_field, ((0, 0), (0, 0), (1, 1)))
    center = padded_field[:, 1:-1, :]
    neighbours = (
        padded_field[:, 2:, :] + padded_field[:, :-2, :] + sided[:, 1:-1, 2:] + sided[:, 1:-1, :-2]
    )
    return (reaction + 4.0) * center - neighbours


def per_device(sensitivity, precision, reaction, load):
    rows, params = load.shape
    strip_rows, columns = reaction.shape
    obs = sensitivity.shape[1]
    strip = lax.axis_index(TILE)
    strips = lax.axis_size(TILE)
    halves = strips // rows
    piece = obs // halves
    lanes = piece // 2
    reaction_deep = with_halo(reaction, 0, 1)
    positions = jnp.arange(strip_rows + 2)
    inside = jnp.logical_and(
        jnp.logical_or(positions > 0, strip > 0),
        jnp.logical_or(positions < strip_rows + 1, strip < strips - 1),
    )
    inside_mask = inside.astype(F32)[None, :, None]
    own_precision = lax.dynamic_index_in_dim(
        precision.reshape(halves, 2, lanes), strip % halves, 0, keepdims=False
    )

    def smoothed(field):
        grid = field.reshape(rows, strip_rows, columns)
        once = stencil_rows(with_halo(grid, 1, 2), reaction_deep) * inside_mask
        return once, stencil_rows(once, reaction).reshape(field.shape)

    def exchanged(tiles):
        return lax.all_to_all(tiles, TILE, 0, 0, tiled=True)

    def observed(field):
        partial = jnp.dot(field.astype(BF16), sensitivity, preferred_element_type=F32)
        return partial.astype(BF16).reshape(strips, 2, lanes)

    def projected(weighted):
        half = lax.dot_general(
            weighted.reshape(rows, obs), sensitivity, (((1,), (1,)), ((), ())), preferred_element_type=F32
        )
        return half + lax.ppermute(half, "rhs", SWAP)

    def to_all(tile):
        return exchanged(jnp.broadcast_to(tile[None], (strips, *tile.shape)))

    _, prior = smoothed(load)
    predicted = exchanged(observed(load)).astype(F32).sum(axis=0)
    weighted = (own_precision * predicted).astype(BF16)
    image = projected(to_all(weighted)) + prior

    once, prior = smoothed(image)
    own_once = once[:, 1:-1, :]
    bent = jnp.sum(own_once * own_once, axis=(1, 2))
    sums = jnp.stack(
        [jnp.sum(load * load, axis=1), jnp.sum(load * image, axis=1), jnp.sum(image * image, axis=1)], axis=-1
    )
    terms = split3(sums).reshape(rows, 9)
    terms = jnp.pad(terms, ((0, 0), (0, 119)))
    terms = jnp.broadcast_to(terms[:, None, None, :], (rows, halves, 2, 128)).reshape(strips, 2, 128)
    arrived = exchanged(jnp.concatenate([observed(image), terms], axis=2)).astype(F32).sum(axis=0)
    predicted = arrived[:, :lanes]
    raised = own_precision * predicted
    own_sums = arrived[0, lanes : lanes + 9].reshape(3, 3).sum(axis=1)
    own_data = jnp.sum(raised * predicted)
    own_terms = split3(jnp.concatenate([own_sums, own_data[None]])).reshape(12)
    bent_terms = split3(bent)[:, :2].reshape(2 * rows)
    message = jnp.concatenate(
        [raised.astype(BF16), jnp.stack([jnp.pad(own_terms, (0, 116)), bent_terms])], axis=1
    )
    received = to_all(message)
    scalars = received[:, :, lanes:].astype(F32)
    bent_sum = jnp.sum(scalars[:, 1, :], axis=0).reshape(rows, 2).sum(axis=1)
    terms = scalars[:, 0, :12].reshape(rows, halves, 4, 3).sum(axis=3)
    bb, bq, qq = terms[:, 0, 0], terms[:, 0, 1], terms[:, 0, 2]
    data = terms[:, :, 3].sum(axis=1)
    qw = data + lax.ppermute(data, "rhs", SWAP) + bent_sum

    alpha = bb / bq
    fresh = bb - 2.0 * alpha * bq + alpha * alpha * qq
    beta = fresh / bb
    grown = 1.0 + beta
    curved = grown * grown * bq - 2.0 * alpha * grown * qq + alpha * alpha * qw
    second = fresh / curved
    near = (alpha + second * grown)[:, None]
    far = (alpha * second)[:, None]

    twice = projected(received[:, :, :lanes]) + prior
    solution = near * load - far * image
    residual = load - near * image + far * twice
    return (solution, residual)


def solution(mesh):
    torus = Mesh(
        mesh.devices.reshape(4, 4, 8, mesh.shape["rhs"]), ("tile_0", "tile_1", "tile_2", "rhs")
    )
    placed = (P(TILE, "rhs"), P("rhs"), P(TILE, None), P(None, TILE))
    return jax.shard_map(
        per_device,
        mesh=torus,
        in_specs=placed,
        out_specs=(P(None, TILE), P(None, TILE)),
        check_vma=False,
    )
```

```python
import jax
import jax.numpy as jnp
from jax import lax
from jax.sharding import Mesh
from jax.sharding import PartitionSpec as P

TILE = ("tile_0", "tile_1", "tile_2")
PLANE = ("tile_0", "tile_1")
LINE = "tile_2"
SWAP = [(0, 1), (1, 0)]
F32, BF16 = jnp.float32, jnp.bfloat16
BLOCK = 8


def packed(x):
    hi = lax.reduce_precision(x, 8, 7)
    mid = lax.reduce_precision(x - hi, 8, 7)
    return jnp.concatenate([hi, mid, x - hi - mid], axis=-1)


def unpacked(x):
    hi, mid, low = jnp.split(x, 3, axis=-1)
    return hi + mid + low


def neighbour_rows(block, dim, width):
    count = lax.axis_size(TILE)
    forward = [(i, i + 1) for i in range(count - 1)]
    backward = [(i + 1, i) for i in range(count - 1)]
    size = block.shape[dim]
    low = lax.ppermute(lax.slice_in_dim(block, size - width, size, axis=dim), TILE, forward)
    high = lax.ppermute(lax.slice_in_dim(block, 0, width, axis=dim), TILE, backward)
    return low, high


def stencil_rows(padded_field, reaction):
    sided = jnp.pad(padded_field, ((0, 0), (0, 0), (1, 1)))
    center = padded_field[:, 1:-1, :]
    neighbours = (
        padded_field[:, 2:, :] + padded_field[:, :-2, :] + sided[:, 1:-1, 2:] + sided[:, 1:-1, :-2]
    )
    return (reaction + 4.0) * center - neighbours


def per_device(sensitivity, precision, reaction, load):
    rows, params = load.shape
    strip_rows, columns = reaction.shape
    obs = sensitivity.shape[1]
    strip = lax.axis_index(TILE)
    strips = lax.axis_size(TILE)
    plane = lax.axis_size(PLANE)
    line = lax.axis_size(LINE)
    groups = rows // BLOCK
    halves = plane // groups
    piece = obs // halves
    positions = jnp.arange(strip_rows + 2)
    inside = jnp.logical_and(
        jnp.logical_or(positions > 0, strip > 0),
        jnp.logical_or(positions < strip_rows + 1, strip < strips - 1),
    )
    inside_mask = inside.astype(F32)[None, :, None]
    own_precision = lax.dynamic_index_in_dim(
        precision.reshape(halves, 1, piece), lax.axis_index(PLANE) % halves, 0, keepdims=False
    )

    def gridded(field):
        return field.reshape(rows, strip_rows, columns)

    def smoothed(field, low, high):
        widened = jnp.concatenate([low, gridded(field), high], axis=1)
        once = stencil_rows(widened, reaction_deep) * inside_mask
        return once, stencil_rows(once, reaction).reshape(field.shape)

    def exchanged(tiles, axis):
        return lax.all_to_all(tiles, axis, 0, 0, tiled=True)

    def summed(tiles, axis):
        return exchanged(tiles.astype(BF16), axis).astype(F32).sum(axis=0)

    def to_all(tile, axis):
        copies = jnp.broadcast_to(tile.astype(BF16)[None], (lax.axis_size(axis), *tile.shape))
        return exchanged(copies, axis)

    def total(tile, axis):
        return to_all(tile, axis).astype(F32).sum(axis=0)

    def observed(field):
        partial = jnp.dot(field.astype(BF16), sensitivity, preferred_element_type=F32)
        tiles = partial.reshape(groups, BLOCK, halves, piece).swapaxes(1, 2)
        return tiles.reshape(plane, BLOCK, piece)

    def projected(tiles):
        weighted = tiles.reshape(groups, halves, BLOCK, piece).swapaxes(1, 2).reshape(rows, obs)
        return lax.dot_general(
            weighted, sensitivity, (((1,), (1,)), ((), ())), preferred_element_type=F32
        )

    def lined(terms):
        return jnp.pad(terms, ((0, 0),) * (terms.ndim - 1) + ((0, 128 - terms.shape[-1]),))

    reaction_low, reaction_high = neighbour_rows(reaction, 0, 1)
    reaction_deep = jnp.concatenate([reaction_low, reaction, reaction_high], axis=0)
    low, high = neighbour_rows(gridded(load), 1, 2)
    tiles, low, high = lax.optimization_barrier((observed(load), low, high))
    _, prior = smoothed(load, low, high)
    predicted = total(summed(tiles, PLANE), LINE)
    half = projected(to_all(own_precision * predicted, PLANE))
    image = half + lax.ppermute(half, "rhs", SWAP) + prior

    low, high = neighbour_rows(gridded(image), 1, 2)
    sums = jnp.stack(
        [jnp.sum(load * load, axis=1), jnp.sum(load * image, axis=1), jnp.sum(image * image, axis=1)], axis=-1
    )
    terms = lined(packed(sums)).reshape(groups, 1, BLOCK, 128)
    terms = jnp.broadcast_to(terms, (groups, halves, BLOCK, 128)).reshape(plane, BLOCK, 128)
    arrived = summed(jnp.concatenate([observed(image), terms], axis=2), PLANE)
    arrived, low, high = lax.optimization_barrier((arrived, low, high))
    once, prior = smoothed(image, low, high)
    bent = jnp.sum(once[:, 1:-1, :] ** 2, axis=(1, 2)).reshape(groups, BLOCK)
    terms = jnp.concatenate([packed(unpacked(arrived[:, piece : piece + 9])), packed(bent)], axis=1)
    arrived = total(jnp.concatenate([arrived[:, :piece], lined(terms)], axis=1), LINE)
    predicted = arrived[:, :piece]
    raised = own_precision * predicted
    data = jnp.sum(raised * predicted, axis=1, keepdims=True)
    row_sums = unpacked(arrived[:, piece : piece + 9])
    bent = unpacked(arrived[:, piece + 9 : piece + 9 + 3 * BLOCK])
    terms = jnp.concatenate([packed(jnp.concatenate([row_sums, data], axis=1)), packed(bent)], axis=1)
    received = to_all(jnp.concatenate([raised, lined(terms)], axis=1), PLANE)
    scalars = received[:, :, piece:].astype(F32)
    bent = unpacked(jnp.sum(scalars[:, :, 12 : 12 + 3 * BLOCK], axis=0)).reshape(rows)
    terms = unpacked(scalars[:, :, :12]).reshape(groups, halves, BLOCK, 4)
    bb, bq, qq = (terms[:, 0, :, i].reshape(rows) for i in range(3))
    data = terms[:, :, :, 3].sum(axis=1).reshape(rows)
    qw = data + lax.ppermute(data, "rhs", SWAP) + bent

    alpha = bb / bq
    fresh = bb - 2.0 * alpha * bq + alpha * alpha * qq
    beta = fresh / bb
    grown = 1.0 + beta
    curved = grown * grown * bq - 2.0 * alpha * grown * qq + alpha * alpha * qw
    second = fresh / curved
    near = (alpha + second * grown)[:, None]
    far = (alpha * second)[:, None]

    half = projected(received[:, :, :piece])
    twice = half + lax.ppermute(half, "rhs", SWAP) + prior
    solution = near * load - far * image
    residual = load - near * image + far * twice
    return (solution, residual)


def solution(mesh):
    torus = Mesh(
        mesh.devices.reshape(4, 4, 8, mesh.shape["rhs"]), ("tile_0", "tile_1", "tile_2", "rhs")
    )
    placed = (P(TILE, "rhs"), P("rhs"), P(TILE, None), P(None, TILE))
    return jax.shard_map(
        per_device,
        mesh=torus,
        in_specs=placed,
        out_specs=(P(None, TILE), P(None, TILE)),
        check_vma=False,
    )
```

```python
import functools

import jax
import jax.numpy as jnp
from jax import lax
from jax.experimental import pallas as pl
from jax.experimental.pallas import tpu as pltpu
from jax.sharding import Mesh
from jax.sharding import PartitionSpec as P

TILE = ("tile_0", "tile_1", "tile_2")
PLANE = ("tile_0", "tile_1")
LINE = "tile_2"
SWAP = [(0, 1), (1, 0)]
F32, BF16 = jnp.float32, jnp.bfloat16
BLOCK = 8
LANES = 128
SLOTS = 16
DATA, BENT = 3, 4
PRIOR_CORE = 1


def from_neighbours(lower, upper):
    strips, cores = lax.axis_size(TILE), lax.axis_size("rhs")
    up = [(i * cores + PRIOR_CORE, (i + 1) * cores + PRIOR_CORE) for i in range(strips - 1)]
    down = [(target, source) for source, target in up]
    axes = (*TILE, "rhs")
    return lax.ppermute(upper, axes, up), lax.ppermute(lower, axes, down)


def moved(x, lanes):
    return pltpu.roll(x, lanes % LANES, 1)


def lane_of(x):
    return lax.broadcasted_iota(jnp.int32, x.shape, 1)


def packed(x):
    x = jnp.where(lane_of(x) < SLOTS, x, 0.0)
    hi = x.astype(BF16).astype(F32)
    mid = (x - hi).astype(BF16).astype(F32)
    return hi + moved(mid, SLOTS) + moved(x - hi - mid, 2 * SLOTS)


def unpacked(x):
    return x + moved(x, -SLOTS) + moved(x, -2 * SLOTS)


def forward_kernel(with_terms, *refs):
    if with_terms:
        field, load, sensitivity, tiles, total = refs
    else:
        field, sensitivity, tiles, total = refs
    rows, obs = total.shape
    groups = rows // BLOCK
    halves = tiles.shape[0] // groups
    piece = obs // halves
    total[...] = jnp.dot(field[...].astype(BF16), sensitivity[...], preferred_element_type=F32)
    for g in range(groups):
        block = slice(g * BLOCK, (g + 1) * BLOCK)
        if with_terms:
            x, y = load[block, :], field[block, :]
            sums = [jnp.sum(p, axis=1, keepdims=True) for p in (x * x, x * y, y * y)]
            lane = lax.broadcasted_iota(jnp.int32, (BLOCK, LANES), 1)
            line = jnp.zeros((BLOCK, LANES), F32)
            for i, value in enumerate(sums):
                line = jnp.where(lane == i, value, line)
            line = packed(line).astype(BF16)
        for h in range(halves):
            tiles[g * halves + h, :, :piece] = total[block, h * piece : (h + 1) * piece].astype(BF16)
            if with_terms:
                tiles[g * halves + h, :, piece:] = line


def added(tiles, part):
    count = tiles.shape[0]
    found = tiles[0, :, part].astype(F32)
    for i in range(1, count):
        found = found + tiles[i, :, part].astype(F32)
    return found


def sent(tile, part, copies):
    for i in range(copies.shape[0]):
        copies[i, :, part] = tile.astype(BF16)


def middle_kernel(piece, *refs):
    tiles, copies = refs[0], refs[-1]
    sent(added(tiles, slice(0, piece)), slice(0, piece), copies)
    if len(refs) == 3:
        terms = slice(piece, piece + LANES)
        line = unpacked(added(tiles, terms))
        line = jnp.where(lane_of(line) < BENT, line, refs[1][...])
        sent(packed(line), terms, copies)


def raised_kernel(piece, tiles, precision, copies):
    predicted = added(tiles, slice(0, piece))
    raised = precision[...] * predicted
    sent(raised, slice(0, piece), copies)
    if tiles.shape[2] > piece:
        terms = slice(piece, piece + LANES)
        line = unpacked(added(tiles, terms))
        data = jnp.sum(raised * predicted, axis=1, keepdims=True)
        line = jnp.where(lane_of(line) == DATA, data, line)
        sent(packed(line), terms, copies)


def back_kernel(piece, tiles, sensitivity, prior, back, wide, turned):
    params = sensitivity.shape[0]
    rows = back.shape[0]
    groups = rows // BLOCK
    halves = tiles.shape[0] // groups
    wide[rows:, :] = jnp.zeros((wide.shape[0] - rows, wide.shape[1]), F32)
    for g in range(groups):
        for h in range(halves):
            block = tiles[g * halves + h, :, :piece].astype(F32)
            wide[g * BLOCK : (g + 1) * BLOCK, h * piece : (h + 1) * piece] = block
    turned[...] = wide[...].T.astype(BF16)
    depth = 256
    for c in range(params // depth):
        part = slice(c * depth, (c + 1) * depth)
        product = jnp.dot(sensitivity[part, :], turned[...], preferred_element_type=F32)
        back[:, part] = product.T[:rows] + prior[:, part]
    if tiles.shape[2] > piece:
        found = [unpacked(tiles[q, :, piece:].astype(F32)) for q in range(tiles.shape[0])]
        spread = sum(found[1:], found[0])
        for g in range(groups):
            own = found[g * halves : (g + 1) * halves]
            lane = lane_of(spread)
            line = jnp.where(lane == DATA, sum(own[1:], own[0]), own[0])
            line = jnp.where(lane == BENT, moved(spread, -g), line)
            back[g * BLOCK : (g + 1) * BLOCK, params:] = line


def prior_kernel(field, low, high, sides, reaction, prior, bent):
    rows, params = field.shape
    strip_rows = params // LANES
    lane = lax.broadcasted_iota(jnp.int32, (BLOCK, LANES), 1)
    first, last = lane == 0, lane == LANES - 1
    bent_tile = jnp.zeros((BLOCK, LANES), F32)

    def wide(row):
        return jnp.broadcast_to(row, (BLOCK, LANES))

    def applied(above, here, below, weight):
        left = jnp.where(first, 0.0, moved(here, 1))
        right = jnp.where(last, 0.0, moved(here, -1))
        return weight * here - (above + below + left + right)

    weights = [wide(sides[0:1, :] + 4.0)]
    weights += [wide(reaction[i : i + 1, :] + 4.0) for i in range(strip_rows)]
    weights += [wide(sides[1:2, :] + 4.0)]
    has_low, has_high, active = (wide(sides[i : i + 1, :]) for i in (2, 3, 4))
    for g in range(rows // BLOCK):
        block = slice(g * BLOCK, (g + 1) * BLOCK)
        q = [low[block, i * LANES : (i + 1) * LANES] for i in range(2)]
        q += [field[block, i * LANES : (i + 1) * LANES] for i in range(strip_rows)]
        q += [high[block, i * LANES : (i + 1) * LANES] for i in range(2)]
        once = [applied(q[i], q[i + 1], q[i + 2], weights[i]) for i in range(strip_rows + 2)]
        once[0] = once[0] * has_low
        once[-1] = once[-1] * has_high
        squares = once[1] * once[1]
        for i in range(2, strip_rows + 1):
            squares = squares + once[i] * once[i]
        total = jnp.sum(squares, axis=1, keepdims=True)
        bent_tile = jnp.where(lane == BENT + g, total, bent_tile)
        for i in range(strip_rows):
            twice = applied(once[i], once[i + 1], once[i + 2], weights[i + 1])
            prior[block, i * LANES : (i + 1) * LANES] = twice * active
    bent[...] = bent_tile * active


def called(kernel, out_shape, operands, scratch=(), flops=10**6):
    vmem = pl.BlockSpec(memory_space=pltpu.VMEM)
    return pl.pallas_call(
        kernel,
        out_shape=out_shape,
        in_specs=[vmem] * len(operands),
        out_specs=jax.tree.map(lambda _: vmem, out_shape),
        scratch_shapes=list(scratch),
        compiler_params=pltpu.CompilerParams(vmem_limit_bytes=16 * 2**20),
        cost_estimate=pl.CostEstimate(flops=flops, bytes_accessed=10**6, transcendentals=0),
    )(*operands)


def per_device(sensitivity, precision, reaction, load):
    rows, params = load.shape
    _, columns = reaction.shape
    obs = sensitivity.shape[1]
    strip = lax.axis_index(TILE)
    strips = lax.axis_size(TILE)
    plane = lax.axis_size(PLANE)
    line = lax.axis_size(LINE)
    groups = rows // BLOCK
    halves = plane // groups
    piece = obs // halves
    flops = 2 * rows * params * obs
    own_precision = lax.dynamic_slice_in_dim(
        precision[None, :], (lax.axis_index(PLANE) % halves) * piece, piece, axis=1
    )

    active = lax.axis_index("rhs") == PRIOR_CORE
    present = jnp.stack([strip > 0, strip < strips - 1, active]).astype(F32)
    present = jnp.broadcast_to(present[:, None], (3, columns))

    def smoothed(field, low, high, sides):
        return called(
            prior_kernel,
            (jax.ShapeDtypeStruct((rows, params), F32), jax.ShapeDtypeStruct((BLOCK, LANES), F32)),
            (field, low, high, sides, reaction),
        )

    def exchanged(tiles, axis):
        return lax.all_to_all(tiles, axis, 0, 0, tiled=True)

    def observed(operands, width):
        return called(
            functools.partial(forward_kernel, width > piece),
            jax.ShapeDtypeStruct((plane, BLOCK, width), BF16),
            operands,
            [pltpu.VMEM((rows, obs), F32)],
            flops,
        )

    def middle(tiles, *more):
        shape = jax.ShapeDtypeStruct((line, BLOCK, tiles.shape[2]), BF16)
        return called(functools.partial(middle_kernel, piece), shape, (tiles, *more))

    def raised(tiles):
        shape = jax.ShapeDtypeStruct((plane, BLOCK, tiles.shape[2]), BF16)
        return called(functools.partial(raised_kernel, piece), shape, (tiles, own_precision))

    def projected(tiles, prior):
        return called(
            functools.partial(back_kernel, piece),
            jax.ShapeDtypeStruct((rows, params + tiles.shape[2] - piece), F32),
            (tiles, sensitivity, prior),
            [pltpu.VMEM((LANES, obs), F32), pltpu.VMEM((obs, LANES), BF16)],
            flops,
        )

    edge = 2 * columns
    above, below = (
        jnp.concatenate([part, jnp.pad(own, ((0, BLOCK - 1), (0, columns)))], axis=0)
        for part, own in ((load[:, :edge], reaction[:1]), (load[:, params - edge :], reaction[-1:]))
    )
    low, high = from_neighbours(above, below)
    tiles = jnp.dot(load.astype(BF16), sensitivity, preferred_element_type=F32).astype(BF16)
    tiles = tiles.reshape(groups, BLOCK, halves, piece).swapaxes(1, 2).reshape(plane, BLOCK, piece)
    sides = jnp.concatenate([low[rows : rows + 1, :columns], high[rows : rows + 1, :columns], present], axis=0)
    sides = jnp.pad(sides, ((0, BLOCK - sides.shape[0]), (0, 0)))
    prior, _ = smoothed(load, low, high, sides)
    tiles, own_precision, sides, prior = lax.optimization_barrier((tiles, own_precision, sides, prior))
    arrived = exchanged(middle(exchanged(tiles, PLANE)), LINE)
    received = exchanged(raised(arrived), PLANE)
    half = projected(received, prior)
    image = half + lax.ppermute(half, "rhs", SWAP)

    low, high = from_neighbours(image[:, :edge], image[:, params - edge :])
    tiles = observed((image, load, sensitivity), piece + LANES)
    tiles, low, high = lax.optimization_barrier((tiles, low, high))
    arrived = exchanged(tiles, PLANE)
    arrived, low, high = lax.optimization_barrier((arrived, low, high))
    prior, bent = smoothed(image, low, high, sides)
    tiles, prior = lax.optimization_barrier((middle(arrived, bent), prior))
    arrived = exchanged(tiles, LINE)
    received = exchanged(raised(arrived), PLANE)
    half = projected(received, prior)
    other = lax.ppermute(half, "rhs", SWAP)
    bb, bq, qq, data, bent = (half[:, params + i] for i in range(5))
    qw = data + other[:, params + DATA] + (bent + other[:, params + BENT])

    alpha = bb / bq
    fresh = bb - 2.0 * alpha * bq + alpha * alpha * qq
    beta = fresh / bb
    grown = 1.0 + beta
    curved = grown * grown * bq - 2.0 * alpha * grown * qq + alpha * alpha * qw
    second = fresh / curved
    near = (alpha + second * grown)[:, None]
    far = (alpha * second)[:, None]

    twice = half[:, :params] + other[:, :params]
    solution = near * load - far * image
    residual = load - near * image + far * twice
    return (solution, residual)


def solution(mesh):
    torus = Mesh(
        mesh.devices.reshape(4, 4, 8, mesh.shape["rhs"]), ("tile_0", "tile_1", "tile_2", "rhs")
    )
    placed = (P(TILE, "rhs"), P("rhs"), P(TILE, None), P(None, TILE))

    return jax.shard_map(
        per_device,
        mesh=torus,
        in_specs=placed,
        out_specs=(P(None, TILE), P(None, TILE)),
        check_vma=False,
    )
```

```python
import functools

import jax
import jax.numpy as jnp
from jax import lax
from jax.experimental import pallas as pl
from jax.experimental.pallas import tpu as pltpu
from jax.sharding import Mesh
from jax.sharding import PartitionSpec as P

TILE = ("tile_0", "tile_1", "tile_2")
PLANE = ("tile_0", "tile_1")
LINE = "tile_2"
SWAP = [(0, 1), (1, 0)]
F32, BF16 = jnp.float32, jnp.bfloat16
BLOCK = 8
LANES = 128
SLOTS = 16
DATA, BENT = 3, 4


def links(core, step):
    strips, cores = lax.axis_size(TILE), lax.axis_size("rhs")
    pairs = [(i, i + step) for i in range(strips) if 0 <= i + step < strips]
    return [(source * cores + core, target * cores + core) for source, target in pairs]


def passed(rows, pairs):
    return lax.ppermute(rows, (*TILE, "rhs"), pairs)


def moved(x, lanes):
    return pltpu.roll(x, lanes % LANES, 1)


def lane_of(x):
    return lax.broadcasted_iota(jnp.int32, x.shape, 1)


def packed(x):
    x = jnp.where(lane_of(x) < SLOTS, x, 0.0)
    hi = x.astype(BF16).astype(F32)
    mid = (x - hi).astype(BF16).astype(F32)
    return hi + moved(mid, SLOTS) + moved(x - hi - mid, 2 * SLOTS)


def unpacked(x):
    return x + moved(x, -SLOTS) + moved(x, -2 * SLOTS)


def forward_kernel(with_terms, *refs):
    if with_terms:
        field, load, sensitivity, tiles, total = refs
    else:
        field, sensitivity, tiles, total = refs
    rows, obs = total.shape
    groups = rows // BLOCK
    halves = tiles.shape[0] // groups
    piece = obs // halves
    total[...] = jnp.dot(field[...].astype(BF16), sensitivity[...], preferred_element_type=F32)
    for g in range(groups):
        block = slice(g * BLOCK, (g + 1) * BLOCK)
        if with_terms:
            x, y = load[block, :], field[block, :]
            sums = [jnp.sum(p, axis=1, keepdims=True) for p in (x * x, x * y, y * y)]
            lane = lax.broadcasted_iota(jnp.int32, (BLOCK, LANES), 1)
            line = jnp.zeros((BLOCK, LANES), F32)
            for i, value in enumerate(sums):
                line = jnp.where(lane == i, value, line)
            line = packed(line).astype(BF16)
        for h in range(halves):
            tiles[g * halves + h, :, :piece] = total[block, h * piece : (h + 1) * piece].astype(BF16)
            if with_terms:
                tiles[g * halves + h, :, piece:] = line


def added(tiles, part):
    count = tiles.shape[0]
    found = tiles[0, :, part].astype(F32)
    for i in range(1, count):
        found = found + tiles[i, :, part].astype(F32)
    return found


def sent(tile, part, copies):
    for i in range(copies.shape[0]):
        copies[i, :, part] = tile.astype(BF16)


def middle_kernel(piece, *refs):
    tiles, copies = refs[0], refs[-1]
    sent(added(tiles, slice(0, piece)), slice(0, piece), copies)
    if len(refs) == 3:
        terms = slice(piece, piece + LANES)
        line = unpacked(added(tiles, terms))
        line = jnp.where(lane_of(line) < BENT, line, refs[1][...])
        sent(packed(line), terms, copies)


def gather_kernel(tiles, total):
    total[0] = added(tiles, slice(None))


def raised_kernel(piece, tiles, precision, copies):
    predicted = added(tiles, slice(0, piece))
    raised = precision[...] * predicted
    sent(raised, slice(0, piece), copies)
    if tiles.shape[2] > piece:
        terms = slice(piece, piece + LANES)
        line = unpacked(added(tiles, terms))
        data = jnp.sum(raised * predicted, axis=1, keepdims=True)
        line = jnp.where(lane_of(line) == DATA, data, line)
        sent(packed(line), terms, copies)


def back_kernel(piece, tiles, sensitivity, prior, back, wide, turned):
    params = sensitivity.shape[0]
    rows = back.shape[0]
    groups = rows // BLOCK
    halves = tiles.shape[0] // groups
    wide[rows:, :] = jnp.zeros((wide.shape[0] - rows, wide.shape[1]), F32)
    for g in range(groups):
        for h in range(halves):
            block = tiles[g * halves + h, :, :piece].astype(F32)
            wide[g * BLOCK : (g + 1) * BLOCK, h * piece : (h + 1) * piece] = block
    turned[...] = wide[...].T.astype(BF16)
    depth = 256
    for c in range(params // depth):
        part = slice(c * depth, (c + 1) * depth)
        product = jnp.dot(sensitivity[part, :], turned[...], preferred_element_type=F32)
        back[:, part] = product.T[:rows] + prior[:, part]
    if tiles.shape[2] > piece:
        found = [unpacked(tiles[q, :, piece:].astype(F32)) for q in range(tiles.shape[0])]
        spread = sum(found[1:], found[0])
        for g in range(groups):
            own = found[g * halves : (g + 1) * halves]
            lane = lane_of(spread)
            line = jnp.where(lane == DATA, sum(own[1:], own[0]), own[0])
            line = jnp.where(lane == BENT, moved(spread, -g), line)
            back[g * BLOCK : (g + 1) * BLOCK, params:] = line


def prior_kernel(field, low, high, low_line, high_line, reaction, prior, *bent):
    rows, params = field.shape
    strip_rows = params // LANES
    lane = lax.broadcasted_iota(jnp.int32, (BLOCK, LANES), 1)
    first, last = lane == 0, lane == LANES - 1
    bent_tile = jnp.zeros((BLOCK, LANES), F32)

    def wide(row):
        return jnp.broadcast_to(row, (BLOCK, LANES))

    def applied(above, here, below, weight):
        left = jnp.where(first, 0.0, moved(here, 1))
        right = jnp.where(last, 0.0, moved(here, -1))
        return weight * here - (above + below + left + right)

    strip, upward = lax.axis_index(TILE), lax.axis_index("rhs") == 1
    has_low = jnp.where(strip > 0, 1.0, 0.0)
    has_high = jnp.where(strip < lax.axis_size(TILE) - 1, 1.0, 0.0)
    own_factor = jnp.where(upward, 1.0, 0.0)
    weights = [low_line[...]]
    weights += [reaction[i : i + 1, :] for i in range(strip_rows)]
    weights += [high_line[...]]
    weights = [wide(row + 4.0) for row in weights]
    for g in range(rows // BLOCK):
        block = slice(g * BLOCK, (g + 1) * BLOCK)
        own = [field[block, i * LANES : (i + 1) * LANES] for i in range(strip_rows)]
        lower, upper = ([e[block, i * LANES : (i + 1) * LANES] for i in range(2)] for e in (low, high))
        q = [row * own_factor for row in (*lower, *own, *upper)]
        once = [applied(q[i], q[i + 1], q[i + 2], weights[i]) for i in range(strip_rows + 2)]
        once[0] = once[0] * has_low
        once[-1] = once[-1] * has_high
        if bent:
            squares = once[1] * once[1]
            for i in range(2, strip_rows + 1):
                squares = squares + once[i] * once[i]
            total = jnp.sum(squares, axis=1, keepdims=True)
            bent_tile = jnp.where(lane == BENT + g, total, bent_tile)
        for i in range(strip_rows):
            twice = applied(once[i], once[i + 1], once[i + 2], weights[i + 1])
            prior[block, i * LANES : (i + 1) * LANES] = twice
    if bent:
        bent[0][...] = bent_tile


def called(kernel, out_shape, operands, scratch=(), flops=10**6):
    vmem = pl.BlockSpec(memory_space=pltpu.VMEM)
    return pl.pallas_call(
        kernel,
        out_shape=out_shape,
        in_specs=[vmem] * len(operands),
        out_specs=jax.tree.map(lambda _: vmem, out_shape),
        scratch_shapes=list(scratch),
        compiler_params=pltpu.CompilerParams(vmem_limit_bytes=16 * 2**20),
        cost_estimate=pl.CostEstimate(flops=flops, bytes_accessed=10**6, transcendentals=0),
    )(*operands)


def per_device(sensitivity, precision, reaction, load):
    rows, params = load.shape
    _, columns = reaction.shape
    obs = sensitivity.shape[1]
    plane = lax.axis_size(PLANE)
    line = lax.axis_size(LINE)
    groups = rows // BLOCK
    halves = plane // groups
    piece = obs // halves
    flops = 2 * rows * params * obs
    own_precision = lax.dynamic_slice_in_dim(
        precision[None, :], (lax.axis_index(PLANE) % halves) * piece, piece, axis=1
    )

    def smoothed(field, low, high, with_bent):
        prior = jax.ShapeDtypeStruct((rows, params), F32)
        bent = jax.ShapeDtypeStruct((BLOCK, LANES), F32)
        shape = (prior, bent) if with_bent else (prior,)
        return called(prior_kernel, shape, (field, low, high, low_line, high_line, reaction))

    def exchanged(tiles, axis):
        return lax.all_to_all(tiles, axis, 0, 0, tiled=True)

    def observed(operands, width):
        return called(
            functools.partial(forward_kernel, width > piece),
            jax.ShapeDtypeStruct((plane, BLOCK, width), BF16),
            operands,
            [pltpu.VMEM((rows, obs), F32)],
            flops,
        )

    def middle(tiles, *more):
        shape = jax.ShapeDtypeStruct((line, BLOCK, tiles.shape[2]), BF16)
        return called(functools.partial(middle_kernel, piece), shape, (tiles, *more))

    def raised(tiles, own_precision):
        shape = jax.ShapeDtypeStruct((plane, BLOCK, tiles.shape[2]), BF16)
        return called(functools.partial(raised_kernel, piece), shape, (tiles, own_precision))

    def projected(tiles, prior):
        return called(
            functools.partial(back_kernel, piece),
            jax.ShapeDtypeStruct((rows, params + tiles.shape[2] - piece), F32),
            (tiles, sensitivity, prior),
            [pltpu.VMEM((LANES, obs), F32), pltpu.VMEM((obs, LANES), BF16)],
            flops,
        )

    edge = 2 * columns

    def with_reaction(part, own):
        return jnp.concatenate([part, jnp.pad(own, ((0, BLOCK - 1), (0, columns)))], axis=0)

    low = passed(with_reaction(load[:, params - edge :], reaction[-1:]), links(1, 1))
    high = passed(with_reaction(load[:, :edge], reaction[:1]), links(1, -1))
    tiles = observed((load, sensitivity), piece)
    low_line, high_line = (e[rows : rows + 1, :columns] for e in (low, high))
    (prior,) = smoothed(load, low, high, False)
    tiles, own_precision, prior, low_line, high_line = lax.optimization_barrier(
        (tiles, own_precision, prior, low_line, high_line)
    )
    tiles = middle(exchanged(tiles, PLANE))
    arrived = exchanged(tiles, LINE)
    received = exchanged(raised(arrived, own_precision), PLANE)
    half = projected(received, prior)
    image = half + lax.ppermute(half, "rhs", SWAP)

    low = passed(image[:, params - edge :], links(1, 1))
    high = passed(image[:, :edge], links(1, -1))
    tiles = observed((image, load, sensitivity), piece + LANES)
    arrived = exchanged(tiles, PLANE)
    shape = jax.ShapeDtypeStruct((1, *arrived.shape[1:]), F32)
    arrived = called(gather_kernel, shape, (arrived,))
    arrived, low, high = lax.optimization_barrier((arrived, low, high))
    prior, bent = smoothed(image, low, high, True)
    tiles, prior = lax.optimization_barrier((middle(arrived, bent), prior))
    arrived = exchanged(tiles, LINE)
    received = exchanged(raised(arrived, own_precision), PLANE)
    half = projected(received, prior)
    other = lax.ppermute(half, "rhs", SWAP)
    bb, bq, qq, data, bent = (half[:, params + i] for i in range(5))
    qw = data + other[:, params + DATA] + (bent + other[:, params + BENT])

    alpha = bb / bq
    fresh = bb - 2.0 * alpha * bq + alpha * alpha * qq
    beta = fresh / bb
    grown = 1.0 + beta
    curved = grown * grown * bq - 2.0 * alpha * grown * qq + alpha * alpha * qw
    second = fresh / curved
    near = (alpha + second * grown)[:, None]
    far = (alpha * second)[:, None]

    twice = half[:, :params] + other[:, :params]
    solution = near * load - far * image
    residual = load - near * image + far * twice
    return (solution, residual)


def solution(mesh):
    torus = Mesh(
        mesh.devices.reshape(4, 4, 8, mesh.shape["rhs"]), ("tile_0", "tile_1", "tile_2", "rhs")
    )
    placed = (P(TILE, "rhs"), P("rhs"), P(TILE, None), P(None, TILE))

    return jax.shard_map(
        per_device,
        mesh=torus,
        in_specs=placed,
        out_specs=(P(None, TILE), P(None, TILE)),
        check_vma=False,
    )
```

```python
import functools

import jax
import jax.numpy as jnp
from jax import lax
from jax.experimental import pallas as pl
from jax.experimental.pallas import tpu as pltpu
from jax.sharding import Mesh
from jax.sharding import PartitionSpec as P

TILE = ("tile_0", "tile_1", "tile_2")
PLANE = ("tile_0", "tile_1")
LINE = "tile_2"
SWAP = [(0, 1), (1, 0)]
F32, BF16 = jnp.float32, jnp.bfloat16
BLOCK = 8
LANES = 128
SLOTS = 16
DATA, BENT = 3, 4


def links(core, step):
    strips, cores = lax.axis_size(TILE), lax.axis_size("rhs")
    pairs = [(i, i + step) for i in range(strips) if 0 <= i + step < strips]
    return [(source * cores + core, target * cores + core) for source, target in pairs]


def passed(rows, pairs):
    return lax.ppermute(rows, (*TILE, "rhs"), pairs)


def moved(x, lanes):
    return pltpu.roll(x, lanes % LANES, 1)


def lane_of(x):
    return lax.broadcasted_iota(jnp.int32, x.shape, 1)


def packed(x):
    x = jnp.where(lane_of(x) < SLOTS, x, 0.0)
    hi = x.astype(BF16).astype(F32)
    mid = (x - hi).astype(BF16).astype(F32)
    return hi + moved(mid, SLOTS) + moved(x - hi - mid, 2 * SLOTS)


def unpacked(x):
    return x + moved(x, -SLOTS) + moved(x, -2 * SLOTS)


def forward_kernel(with_terms, *refs):
    if with_terms:
        field, load, sensitivity, tiles, total = refs
    else:
        field, sensitivity, tiles, total = refs
    rows, obs = total.shape
    groups = rows // BLOCK
    halves = tiles.shape[0] // groups
    piece = obs // halves
    total[...] = jnp.dot(field[...].astype(BF16), sensitivity[...], preferred_element_type=F32)
    for g in range(groups):
        block = slice(g * BLOCK, (g + 1) * BLOCK)
        if with_terms:
            x, y = load[block, :], field[block, :]
            sums = [jnp.sum(p, axis=1, keepdims=True) for p in (x * x, x * y, y * y)]
            lane = lax.broadcasted_iota(jnp.int32, (BLOCK, LANES), 1)
            line = jnp.zeros((BLOCK, LANES), F32)
            for i, value in enumerate(sums):
                line = jnp.where(lane == i, value, line)
            line = packed(line).astype(BF16)
        for h in range(halves):
            tiles[g * halves + h, :, :piece] = total[block, h * piece : (h + 1) * piece].astype(BF16)
            if with_terms:
                tiles[g * halves + h, :, piece:] = line


def added(tiles, part):
    count = tiles.shape[0]
    found = tiles[0, :, part].astype(F32)
    for i in range(1, count):
        found = found + tiles[i, :, part].astype(F32)
    return found


def sent(tile, part, copies):
    for i in range(copies.shape[0]):
        copies[i, :, part] = tile.astype(BF16)


def middle_kernel(piece, *refs):
    tiles, copies = refs[0], refs[-1]
    sent(added(tiles, slice(0, piece)), slice(0, piece), copies)
    if len(refs) == 3:
        terms = slice(piece, piece + LANES)
        line = unpacked(added(tiles, terms))
        line = jnp.where(lane_of(line) < BENT, line, refs[1][...])
        sent(packed(line), terms, copies)


def relay_kernel(tiles, out):
    out[...] = tiles[...]


def gather_kernel(tiles, total):
    total[0] = added(tiles, slice(None))


def raised_kernel(piece, tiles, precision, copies):
    predicted = added(tiles, slice(0, piece))
    half = lax.axis_index(PLANE) % (precision.shape[0] // piece)
    own = precision[:piece]
    for i in range(1, precision.shape[0] // piece):
        own = jnp.where(half == i, precision[i * piece : (i + 1) * piece], own)
    raised = own.reshape(1, piece) * predicted
    sent(raised, slice(0, piece), copies)
    if tiles.shape[2] > piece:
        terms = slice(piece, piece + LANES)
        line = unpacked(added(tiles, terms))
        data = jnp.sum(raised * predicted, axis=1, keepdims=True)
        line = jnp.where(lane_of(line) == DATA, data, line)
        sent(packed(line), terms, copies)


def back_kernel(piece, tiles, sensitivity, prior, back, wide, turned):
    params = sensitivity.shape[0]
    rows = back.shape[0]
    groups = rows // BLOCK
    halves = tiles.shape[0] // groups
    wide[rows:, :] = jnp.zeros((wide.shape[0] - rows, wide.shape[1]), F32)
    for g in range(groups):
        for h in range(halves):
            block = tiles[g * halves + h, :, :piece].astype(F32)
            wide[g * BLOCK : (g + 1) * BLOCK, h * piece : (h + 1) * piece] = block
    turned[...] = wide[...].T.astype(BF16)
    depth = 256
    for c in range(params // depth):
        part = slice(c * depth, (c + 1) * depth)
        product = jnp.dot(sensitivity[part, :], turned[...], preferred_element_type=F32)
        back[:, part] = product.T[:rows] + prior[:, part]
    if tiles.shape[2] > piece:
        found = [unpacked(tiles[q, :, piece:].astype(F32)) for q in range(tiles.shape[0])]
        spread = sum(found[1:], found[0])
        for g in range(groups):
            own = found[g * halves : (g + 1) * halves]
            lane = lane_of(spread)
            line = jnp.where(lane == DATA, sum(own[1:], own[0]), own[0])
            line = jnp.where(lane == BENT, moved(spread, -g), line)
            back[g * BLOCK : (g + 1) * BLOCK, params:] = line


def prior_kernel(field, low, high, low_line, high_line, reaction, prior, *bent):
    rows, params = field.shape
    strip_rows = params // LANES
    lane = lax.broadcasted_iota(jnp.int32, (BLOCK, LANES), 1)
    first, last = lane == 0, lane == LANES - 1
    bent_tile = jnp.zeros((BLOCK, LANES), F32)

    def wide(row):
        return jnp.broadcast_to(row, (BLOCK, LANES))

    def applied(above, here, below, weight):
        left = jnp.where(first, 0.0, moved(here, 1))
        right = jnp.where(last, 0.0, moved(here, -1))
        return weight * here - (above + below + left + right)

    strip, upward = lax.axis_index(TILE), lax.axis_index("rhs") == 1
    has_low = jnp.where(strip > 0, 1.0, 0.0)
    has_high = jnp.where(strip < lax.axis_size(TILE) - 1, 1.0, 0.0)
    own_factor = jnp.where(upward, 1.0, 0.0)
    weights = [low_line[...]]
    weights += [reaction[i : i + 1, :] for i in range(strip_rows)]
    weights += [high_line[...]]
    weights = [wide(row + 4.0) for row in weights]
    for g in range(rows // BLOCK):
        block = slice(g * BLOCK, (g + 1) * BLOCK)
        own = [field[block, i * LANES : (i + 1) * LANES] for i in range(strip_rows)]
        lower, upper = ([e[block, i * LANES : (i + 1) * LANES] for i in range(2)] for e in (low, high))
        q = [row * own_factor for row in (*lower, *own, *upper)]
        once = [applied(q[i], q[i + 1], q[i + 2], weights[i]) for i in range(strip_rows + 2)]
        once[0] = once[0] * has_low
        once[-1] = once[-1] * has_high
        if bent:
            squares = once[1] * once[1]
            for i in range(2, strip_rows + 1):
                squares = squares + once[i] * once[i]
            total = jnp.sum(squares, axis=1, keepdims=True)
            bent_tile = jnp.where(lane == BENT + g, total, bent_tile)
        for i in range(strip_rows):
            twice = applied(once[i], once[i + 1], once[i + 2], weights[i + 1])
            prior[block, i * LANES : (i + 1) * LANES] = twice
    if bent:
        bent[0][...] = bent_tile


def called(kernel, out_shape, operands, scratch=(), flops=10**6):
    vmem = pl.BlockSpec(memory_space=pltpu.VMEM)
    return pl.pallas_call(
        kernel,
        out_shape=out_shape,
        in_specs=[vmem] * len(operands),
        out_specs=jax.tree.map(lambda _: vmem, out_shape),
        scratch_shapes=list(scratch),
        compiler_params=pltpu.CompilerParams(vmem_limit_bytes=16 * 2**20),
        cost_estimate=pl.CostEstimate(flops=flops, bytes_accessed=10**6, transcendentals=0),
    )(*operands)


def per_device(sensitivity, precision, reaction, load):
    rows, params = load.shape
    _, columns = reaction.shape
    obs = sensitivity.shape[1]
    plane = lax.axis_size(PLANE)
    line = lax.axis_size(LINE)
    groups = rows // BLOCK
    halves = plane // groups
    piece = obs // halves
    flops = 2 * rows * params * obs

    def smoothed(field, low, high, with_bent):
        prior = jax.ShapeDtypeStruct((rows, params), F32)
        bent = jax.ShapeDtypeStruct((BLOCK, LANES), F32)
        shape = (prior, bent) if with_bent else (prior,)
        return called(prior_kernel, shape, (field, low, high, low_line, high_line, reaction))

    def exchanged(tiles, axis):
        return lax.all_to_all(tiles, axis, 0, 0, tiled=True)

    def observed(operands, width):
        return called(
            functools.partial(forward_kernel, width > piece),
            jax.ShapeDtypeStruct((plane, BLOCK, width), BF16),
            operands,
            [pltpu.VMEM((rows, obs), F32)],
            flops,
        )

    def middle(tiles, *more):
        shape = jax.ShapeDtypeStruct((line, BLOCK, tiles.shape[2]), BF16)
        return called(functools.partial(middle_kernel, piece), shape, (tiles, *more))

    def raised(tiles):
        shape = jax.ShapeDtypeStruct((plane, BLOCK, tiles.shape[2]), BF16)
        return called(functools.partial(raised_kernel, piece), shape, (tiles, precision))

    def projected(tiles, prior):
        return called(
            functools.partial(back_kernel, piece),
            jax.ShapeDtypeStruct((rows, params + tiles.shape[2] - piece), F32),
            (tiles, sensitivity, prior),
            [pltpu.VMEM((LANES, obs), F32), pltpu.VMEM((obs, LANES), BF16)],
            flops,
        )

    edge = 2 * columns

    def with_reaction(part, own):
        return jnp.concatenate([part, jnp.pad(own, ((0, BLOCK - 1), (0, columns)))], axis=0)

    tiles = observed((load, sensitivity), piece)
    tiles, load, reaction = lax.optimization_barrier((tiles, load, reaction))
    low = passed(with_reaction(load[:, params - edge :], reaction[-1:]), links(1, 1))
    high = passed(with_reaction(load[:, :edge], reaction[:1]), links(1, -1))
    tiles = called(relay_kernel, jax.ShapeDtypeStruct(tiles.shape, BF16), (tiles,))
    tiles = exchanged(tiles, PLANE)
    tiles = middle(tiles)
    tiles, low, high = lax.optimization_barrier((tiles, low, high))
    low_line, high_line = (e[rows : rows + 1, :columns] for e in (low, high))
    (prior,) = smoothed(load, low, high, False)
    tiles, prior, low_line, high_line = lax.optimization_barrier((tiles, prior, low_line, high_line))
    arrived = exchanged(tiles, LINE)
    received = exchanged(raised(arrived), PLANE)
    half = projected(received, prior)
    image = half + lax.ppermute(half, "rhs", SWAP)

    low = passed(image[:, params - edge :], links(1, 1))
    high = passed(image[:, :edge], links(1, -1))
    tiles = observed((image, load, sensitivity), piece + LANES)
    arrived = exchanged(tiles, PLANE)
    shape = jax.ShapeDtypeStruct((1, *arrived.shape[1:]), F32)
    arrived = called(gather_kernel, shape, (arrived,))
    arrived, low, high = lax.optimization_barrier((arrived, low, high))
    prior, bent = smoothed(image, low, high, True)
    tiles, prior = lax.optimization_barrier((middle(arrived, bent), prior))
    arrived = exchanged(tiles, LINE)
    received = exchanged(raised(arrived), PLANE)
    half = projected(received, prior)
    other = lax.ppermute(half, "rhs", SWAP)
    bb, bq, qq, data, bent = (half[:, params + i] for i in range(5))
    qw = data + other[:, params + DATA] + (bent + other[:, params + BENT])

    alpha = bb / bq
    fresh = bb - 2.0 * alpha * bq + alpha * alpha * qq
    beta = fresh / bb
    grown = 1.0 + beta
    curved = grown * grown * bq - 2.0 * alpha * grown * qq + alpha * alpha * qw
    second = fresh / curved
    near = (alpha + second * grown)[:, None]
    far = (alpha * second)[:, None]

    twice = half[:, :params] + other[:, :params]
    solution = near * load - far * image
    residual = load - near * image + far * twice
    return (solution, residual)


def solution(mesh):
    torus = Mesh(
        mesh.devices.reshape(4, 4, 8, mesh.shape["rhs"]), ("tile_0", "tile_1", "tile_2", "rhs")
    )
    placed = (P(TILE, "rhs"), P("rhs"), P(TILE, None), P(None, TILE))

    return jax.shard_map(
        per_device,
        mesh=torus,
        in_specs=placed,
        out_specs=(P(None, TILE), P(None, TILE)),
        check_vma=False,
    )
```

```python
import functools

import jax
import jax.numpy as jnp
from jax import lax
from jax.experimental import pallas as pl
from jax.experimental.pallas import tpu as pltpu
from jax.sharding import Mesh
from jax.sharding import PartitionSpec as P

TILE = ("tile_0", "tile_1", "tile_2")
PLANE = ("tile_0", "tile_1")
LINE = "tile_2"
SWAP = [(0, 1), (1, 0)]
F32, BF16 = jnp.float32, jnp.bfloat16
BLOCK = 8
LANES = 128
SLOTS = 16
DATA, BENT = 3, 4


def links(core, step):
    strips, cores = lax.axis_size(TILE), lax.axis_size("rhs")
    pairs = [(i, i + step) for i in range(strips) if 0 <= i + step < strips]
    return [(source * cores + core, target * cores + core) for source, target in pairs]


def passed(rows, pairs):
    return lax.ppermute(rows, (*TILE, "rhs"), pairs)


def moved(x, lanes):
    return pltpu.roll(x, lanes % LANES, 1)


def lane_of(x):
    return lax.broadcasted_iota(jnp.int32, x.shape, 1)


def packed(x):
    x = jnp.where(lane_of(x) < SLOTS, x, 0.0)
    hi = x.astype(BF16).astype(F32)
    mid = (x - hi).astype(BF16).astype(F32)
    return hi + moved(mid, SLOTS) + moved(x - hi - mid, 2 * SLOTS)


def unpacked(x):
    return x + moved(x, -SLOTS) + moved(x, -2 * SLOTS)


def forward_kernel(with_terms, *refs):
    if with_terms:
        field, load, sensitivity, tiles, total = refs
    else:
        field, sensitivity, tiles, total = refs
    rows, obs = total.shape
    groups = rows // BLOCK
    halves = tiles.shape[0] // groups
    piece = obs // halves
    total[...] = jnp.dot(field[...].astype(BF16), sensitivity[...], preferred_element_type=F32)
    for g in range(groups):
        block = slice(g * BLOCK, (g + 1) * BLOCK)
        if with_terms:
            x, y = load[block, :], field[block, :]
            sums = [jnp.sum(p, axis=1, keepdims=True) for p in (x * x, x * y, y * y)]
            lane = lax.broadcasted_iota(jnp.int32, (BLOCK, LANES), 1)
            line = jnp.zeros((BLOCK, LANES), F32)
            for i, value in enumerate(sums):
                line = jnp.where(lane == i, value, line)
            line = packed(line).astype(BF16)
        for h in range(halves):
            tiles[g * halves + h, :, :piece] = total[block, h * piece : (h + 1) * piece].astype(BF16)
            if with_terms:
                tiles[g * halves + h, :, piece:] = line


def added(tiles, part):
    count = tiles.shape[0]
    found = tiles[0, :, part].astype(F32)
    for i in range(1, count):
        found = found + tiles[i, :, part].astype(F32)
    return found


def sent(tile, part, copies):
    for i in range(copies.shape[0]):
        copies[i, :, part] = tile.astype(BF16)


def middle_kernel(piece, *refs):
    tiles, copies = refs[0], refs[-1]
    sent(added(tiles, slice(0, piece)), slice(0, piece), copies)
    if len(refs) == 3:
        terms = slice(piece, piece + LANES)
        line = unpacked(added(tiles, terms))
        line = jnp.where(lane_of(line) < BENT, line, refs[1][...])
        sent(packed(line), terms, copies)


def relay_kernel(tiles, out):
    out[...] = tiles[...]


def gather_kernel(tiles, total):
    total[0] = added(tiles, slice(None))


def raised_kernel(piece, tiles, precision, copies):
    predicted = added(tiles, slice(0, piece))
    half = lax.axis_index(PLANE) % (precision.shape[0] // piece)
    own = precision[:piece]
    for i in range(1, precision.shape[0] // piece):
        own = jnp.where(half == i, precision[i * piece : (i + 1) * piece], own)
    raised = own.reshape(1, piece) * predicted
    sent(raised, slice(0, piece), copies)
    if tiles.shape[2] > piece:
        terms = slice(piece, piece + LANES)
        line = unpacked(added(tiles, terms))
        data = jnp.sum(raised * predicted, axis=1, keepdims=True)
        line = jnp.where(lane_of(line) == DATA, data, line)
        sent(packed(line), terms, copies)


def back_kernel(piece, tiles, sensitivity, prior, back, wide, turned):
    params = sensitivity.shape[0]
    rows = back.shape[0]
    groups = rows // BLOCK
    halves = tiles.shape[0] // groups
    wide[rows:, :] = jnp.zeros((wide.shape[0] - rows, wide.shape[1]), F32)
    for g in range(groups):
        for h in range(halves):
            block = tiles[g * halves + h, :, :piece].astype(F32)
            wide[g * BLOCK : (g + 1) * BLOCK, h * piece : (h + 1) * piece] = block
    turned[...] = wide[...].T.astype(BF16)
    depth = 256
    for c in range(params // depth):
        part = slice(c * depth, (c + 1) * depth)
        product = jnp.dot(sensitivity[part, :], turned[...], preferred_element_type=F32)
        back[:, part] = product.T[:rows] + prior[:, part]
    if tiles.shape[2] > piece:
        found = [unpacked(tiles[q, :, piece:].astype(F32)) for q in range(tiles.shape[0])]
        spread = sum(found[1:], found[0])
        for g in range(groups):
            own = found[g * halves : (g + 1) * halves]
            lane = lane_of(spread)
            line = jnp.where(lane == DATA, sum(own[1:], own[0]), own[0])
            line = jnp.where(lane == BENT, moved(spread, -g), line)
            back[g * BLOCK : (g + 1) * BLOCK, params:] = line


def prior_kernel(field, low, high, low_line, high_line, reaction, prior, *bent):
    rows, params = field.shape
    strip_rows = params // LANES
    lane = lax.broadcasted_iota(jnp.int32, (BLOCK, LANES), 1)
    first, last = lane == 0, lane == LANES - 1
    bent_tile = jnp.zeros((BLOCK, LANES), F32)

    def wide(row):
        return jnp.broadcast_to(row, (BLOCK, LANES))

    def applied(above, here, below, weight):
        left = jnp.where(first, 0.0, moved(here, 1))
        right = jnp.where(last, 0.0, moved(here, -1))
        return weight * here - (above + below + left + right)

    strip, upward = lax.axis_index(TILE), lax.axis_index("rhs") == 1
    has_low = jnp.where(strip > 0, 1.0, 0.0)
    has_high = jnp.where(strip < lax.axis_size(TILE) - 1, 1.0, 0.0)
    own_factor = jnp.where(upward, 1.0, 0.0)
    weights = [low_line[...]]
    weights += [reaction[i : i + 1, :] for i in range(strip_rows)]
    weights += [high_line[...]]
    weights = [wide(row + 4.0) for row in weights]
    for g in range(rows // BLOCK):
        block = slice(g * BLOCK, (g + 1) * BLOCK)
        own = [field[block, i * LANES : (i + 1) * LANES] for i in range(strip_rows)]
        lower, upper = ([e[block, i * LANES : (i + 1) * LANES] for i in range(2)] for e in (low, high))
        q = [row * own_factor for row in (*lower, *own, *upper)]
        once = [applied(q[i], q[i + 1], q[i + 2], weights[i]) for i in range(strip_rows + 2)]
        once[0] = once[0] * has_low
        once[-1] = once[-1] * has_high
        if bent:
            squares = once[1] * once[1]
            for i in range(2, strip_rows + 1):
                squares = squares + once[i] * once[i]
            total = jnp.sum(squares, axis=1, keepdims=True)
            bent_tile = jnp.where(lane == BENT + g, total, bent_tile)
        for i in range(strip_rows):
            twice = applied(once[i], once[i + 1], once[i + 2], weights[i + 1])
            prior[block, i * LANES : (i + 1) * LANES] = twice
    if bent:
        bent[0][...] = bent_tile


def called(kernel, out_shape, operands, scratch=(), flops=10**6):
    vmem = pl.BlockSpec(memory_space=pltpu.VMEM)
    return pl.pallas_call(
        kernel,
        out_shape=out_shape,
        in_specs=[vmem] * len(operands),
        out_specs=jax.tree.map(lambda _: vmem, out_shape),
        scratch_shapes=list(scratch),
        compiler_params=pltpu.CompilerParams(vmem_limit_bytes=16 * 2**20),
        cost_estimate=pl.CostEstimate(flops=flops, bytes_accessed=10**7, transcendentals=0),
    )(*operands)


def per_device(sensitivity, precision, reaction, load):
    rows, params = load.shape
    _, columns = reaction.shape
    obs = sensitivity.shape[1]
    plane = lax.axis_size(PLANE)
    line = lax.axis_size(LINE)
    groups = rows // BLOCK
    halves = plane // groups
    piece = obs // halves
    flops = 2 * rows * params * obs

    def smoothed(field, low, high, with_bent):
        prior = jax.ShapeDtypeStruct((rows, params), F32)
        bent = jax.ShapeDtypeStruct((BLOCK, LANES), F32)
        shape = (prior, bent) if with_bent else (prior,)
        return called(prior_kernel, shape, (field, low, high, low_line, high_line, reaction))

    def exchanged(tiles, axis):
        return lax.all_to_all(tiles, axis, 0, 0, tiled=True)

    def observed(operands, width):
        return called(
            functools.partial(forward_kernel, width > piece),
            jax.ShapeDtypeStruct((plane, BLOCK, width), BF16),
            operands,
            [pltpu.VMEM((rows, obs), F32)],
            flops,
        )

    def middle(tiles, *more):
        shape = jax.ShapeDtypeStruct((line, BLOCK, tiles.shape[2]), BF16)
        return called(functools.partial(middle_kernel, piece), shape, (tiles, *more))

    def raised(tiles):
        shape = jax.ShapeDtypeStruct((plane, BLOCK, tiles.shape[2]), BF16)
        return called(functools.partial(raised_kernel, piece), shape, (tiles, precision))

    def projected(tiles, prior):
        return called(
            functools.partial(back_kernel, piece),
            jax.ShapeDtypeStruct((rows, params + tiles.shape[2] - piece), F32),
            (tiles, sensitivity, prior),
            [pltpu.VMEM((LANES, obs), F32), pltpu.VMEM((obs, LANES), BF16)],
            flops,
        )

    edge = 2 * columns

    def with_reaction(part, own):
        return jnp.concatenate([part, jnp.pad(own, ((0, BLOCK - 1), (0, columns)))], axis=0)

    tiles = jnp.dot(load.astype(BF16), sensitivity, preferred_element_type=F32).astype(BF16)
    tiles = tiles.reshape(groups, BLOCK, halves, piece).swapaxes(1, 2).reshape(plane, BLOCK, piece)
    tiles, load, reaction = lax.optimization_barrier((tiles, load, reaction))
    low = passed(with_reaction(load[:, params - edge :], reaction[-1:]), links(1, 1))
    high = passed(with_reaction(load[:, :edge], reaction[:1]), links(1, -1))
    tiles = called(relay_kernel, jax.ShapeDtypeStruct(tiles.shape, BF16), (tiles,))
    tiles = exchanged(tiles, PLANE)
    tiles = middle(tiles)
    tiles, low, high = lax.optimization_barrier((tiles, low, high))
    low_line, high_line = (e[rows : rows + 1, :columns] for e in (low, high))
    (prior,) = smoothed(load, low, high, False)
    tiles, prior, low_line, high_line = lax.optimization_barrier((tiles, prior, low_line, high_line))
    arrived = exchanged(tiles, LINE)
    received = exchanged(raised(arrived), PLANE)
    half = projected(received, prior)
    image = half + lax.ppermute(half, "rhs", SWAP)

    low = passed(image[:, params - edge :], links(1, 1))
    high = passed(image[:, :edge], links(1, -1))
    tiles = observed((image, load, sensitivity), piece + LANES)
    arrived = exchanged(tiles, PLANE)
    shape = jax.ShapeDtypeStruct((1, *arrived.shape[1:]), F32)
    arrived = called(gather_kernel, shape, (arrived,))
    arrived, low, high = lax.optimization_barrier((arrived, low, high))
    prior, bent = smoothed(image, low, high, True)
    tiles, prior = lax.optimization_barrier((middle(arrived, bent), prior))
    arrived = exchanged(tiles, LINE)
    received = exchanged(raised(arrived), PLANE)
    half = projected(received, prior)
    other = lax.ppermute(half, "rhs", SWAP)
    bb, bq, qq, data, bent = (half[:, params + i] for i in range(5))
    qw = data + other[:, params + DATA] + (bent + other[:, params + BENT])

    alpha = bb / bq
    fresh = bb - 2.0 * alpha * bq + alpha * alpha * qq
    beta = fresh / bb
    grown = 1.0 + beta
    curved = grown * grown * bq - 2.0 * alpha * grown * qq + alpha * alpha * qw
    second = fresh / curved
    near = (alpha + second * grown)[:, None]
    far = (alpha * second)[:, None]

    twice = half[:, :params] + other[:, :params]
    solution = near * load - far * image
    residual = load - near * image + far * twice
    return (solution, residual)


def solution(mesh):
    torus = Mesh(
        mesh.devices.reshape(4, 4, 8, mesh.shape["rhs"]), ("tile_0", "tile_1", "tile_2", "rhs")
    )
    placed = (P(TILE, "rhs"), P("rhs"), P(TILE, None), P(None, TILE))

    return jax.shard_map(
        per_device,
        mesh=torus,
        in_specs=placed,
        out_specs=(P(None, TILE), P(None, TILE)),
        check_vma=False,
    )
```

```python
import functools

import jax
import jax.numpy as jnp
from jax import lax
from jax.experimental import pallas as pl
from jax.experimental.pallas import tpu as pltpu
from jax.sharding import Mesh
from jax.sharding import PartitionSpec as P

TILE = ("tile_0", "tile_1", "tile_2")
PLANE = ("tile_0", "tile_1")
LINE = "tile_2"
SWAP = [(0, 1), (1, 0)]
F32, BF16 = jnp.float32, jnp.bfloat16
BLOCK = 8
LANES = 128
SLOTS = 16
DATA, BENT = 3, 4


def links(core, step):
    strips, cores = lax.axis_size(TILE), lax.axis_size("rhs")
    pairs = [(i, i + step) for i in range(strips) if 0 <= i + step < strips]
    return [(source * cores + core, target * cores + core) for source, target in pairs]


def passed(rows, pairs):
    return lax.ppermute(rows, (*TILE, "rhs"), pairs)


def moved(x, lanes):
    return pltpu.roll(x, lanes % LANES, 1)


def lane_of(x):
    return lax.broadcasted_iota(jnp.int32, x.shape, 1)


def packed(x):
    x = jnp.where(lane_of(x) < SLOTS, x, 0.0)
    hi = x.astype(BF16).astype(F32)
    mid = (x - hi).astype(BF16).astype(F32)
    return hi + moved(mid, SLOTS) + moved(x - hi - mid, 2 * SLOTS)


def unpacked(x):
    return x + moved(x, -SLOTS) + moved(x, -2 * SLOTS)


def forward_kernel(with_terms, *refs):
    if with_terms:
        field, load, sensitivity, tiles, total = refs
    else:
        field, sensitivity, tiles, total = refs
    rows, obs = total.shape
    groups = rows // BLOCK
    halves = tiles.shape[0] // groups
    piece = obs // halves
    total[...] = jnp.dot(field[...].astype(BF16), sensitivity[...], preferred_element_type=F32)
    for g in range(groups):
        block = slice(g * BLOCK, (g + 1) * BLOCK)
        if with_terms:
            x, y = load[block, :], field[block, :]
            sums = [jnp.sum(p, axis=1, keepdims=True) for p in (x * x, x * y, y * y)]
            lane = lax.broadcasted_iota(jnp.int32, (BLOCK, LANES), 1)
            line = jnp.zeros((BLOCK, LANES), F32)
            for i, value in enumerate(sums):
                line = jnp.where(lane == i, value, line)
            line = packed(line).astype(BF16)
        for h in range(halves):
            tiles[g * halves + h, :, :piece] = total[block, h * piece : (h + 1) * piece].astype(BF16)
            if with_terms:
                tiles[g * halves + h, :, piece:] = line


def added(tiles, part):
    count = tiles.shape[0]
    found = tiles[0, :, part].astype(F32)
    for i in range(1, count):
        found = found + tiles[i, :, part].astype(F32)
    return found


def sent(tile, part, copies):
    for i in range(copies.shape[0]):
        copies[i, :, part] = tile.astype(BF16)


def middle_kernel(piece, *refs):
    tiles, copies = refs[0], refs[-1]
    sent(added(tiles, slice(0, piece)), slice(0, piece), copies)
    if len(refs) == 3:
        terms = slice(piece, piece + LANES)
        line = unpacked(added(tiles, terms))
        line = jnp.where(lane_of(line) < BENT, line, refs[1][...])
        sent(packed(line), terms, copies)


def relay_kernel(tiles, out):
    out[...] = tiles[...]


def gather_kernel(tiles, total):
    total[0] = added(tiles, slice(None))


def raised_kernel(piece, tiles, precision, copies):
    predicted = added(tiles, slice(0, piece))
    half = lax.axis_index(PLANE) % (precision.shape[0] // piece)
    own = precision[:piece]
    for i in range(1, precision.shape[0] // piece):
        own = jnp.where(half == i, precision[i * piece : (i + 1) * piece], own)
    raised = own.reshape(1, piece) * predicted
    sent(raised, slice(0, piece), copies)
    if tiles.shape[2] > piece:
        terms = slice(piece, piece + LANES)
        line = unpacked(added(tiles, terms))
        data = jnp.sum(raised * predicted, axis=1, keepdims=True)
        line = jnp.where(lane_of(line) == DATA, data, line)
        sent(packed(line), terms, copies)


def back_kernel(piece, tiles, sensitivity, prior, back, wide, turned):
    params = sensitivity.shape[0]
    rows = back.shape[0]
    groups = rows // BLOCK
    halves = tiles.shape[0] // groups
    wide[rows:, :] = jnp.zeros((wide.shape[0] - rows, wide.shape[1]), F32)
    for g in range(groups):
        for h in range(halves):
            block = tiles[g * halves + h, :, :piece].astype(F32)
            wide[g * BLOCK : (g + 1) * BLOCK, h * piece : (h + 1) * piece] = block
    turned[...] = wide[...].T.astype(BF16)
    depth = 256
    for c in range(params // depth):
        part = slice(c * depth, (c + 1) * depth)
        product = jnp.dot(sensitivity[part, :], turned[...], preferred_element_type=F32)
        back[:, part] = product.T[:rows] + prior[:, part]
    if tiles.shape[2] > piece:
        found = [unpacked(tiles[q, :, piece:].astype(F32)) for q in range(tiles.shape[0])]
        spread = sum(found[1:], found[0])
        for g in range(groups):
            own = found[g * halves : (g + 1) * halves]
            lane = lane_of(spread)
            line = jnp.where(lane == DATA, sum(own[1:], own[0]), own[0])
            line = jnp.where(lane == BENT, moved(spread, -g), line)
            back[g * BLOCK : (g + 1) * BLOCK, params:] = line


def prior_kernel(field, low, high, low_line, high_line, reaction, prior, *bent):
    rows, params = field.shape
    strip_rows = params // LANES
    lane = lax.broadcasted_iota(jnp.int32, (BLOCK, LANES), 1)
    first, last = lane == 0, lane == LANES - 1
    bent_tile = jnp.zeros((BLOCK, LANES), F32)

    def wide(row):
        return jnp.broadcast_to(row, (BLOCK, LANES))

    def applied(above, here, below, weight):
        left = jnp.where(first, 0.0, moved(here, 1))
        right = jnp.where(last, 0.0, moved(here, -1))
        return weight * here - (above + below + left + right)

    strip, upward = lax.axis_index(TILE), lax.axis_index("rhs") == 1
    has_low = jnp.where(strip > 0, 1.0, 0.0)
    has_high = jnp.where(strip < lax.axis_size(TILE) - 1, 1.0, 0.0)
    own_factor = jnp.where(upward, 1.0, 0.0)
    weights = [low_line[...]]
    weights += [reaction[i : i + 1, :] for i in range(strip_rows)]
    weights += [high_line[...]]
    weights = [wide(row + 4.0) for row in weights]
    for g in range(rows // BLOCK):
        block = slice(g * BLOCK, (g + 1) * BLOCK)
        own = [field[block, i * LANES : (i + 1) * LANES] for i in range(strip_rows)]
        lower, upper = ([e[block, i * LANES : (i + 1) * LANES] for i in range(2)] for e in (low, high))
        q = [*lower, *own, *upper]
        once = [applied(q[i], q[i + 1], q[i + 2], weights[i]) for i in range(strip_rows + 2)]
        once[0] = once[0] * has_low
        once[-1] = once[-1] * has_high
        if bent:
            squares = once[1] * once[1]
            for i in range(2, strip_rows + 1):
                squares = squares + once[i] * once[i]
            total = jnp.sum(squares, axis=1, keepdims=True)
            bent_tile = jnp.where(lane == BENT + g, total, bent_tile)
        for i in range(strip_rows):
            twice = applied(once[i], once[i + 1], once[i + 2], weights[i + 1])
            prior[block, i * LANES : (i + 1) * LANES] = twice * own_factor
    if bent:
        bent[0][...] = bent_tile * own_factor


def called(kernel, out_shape, operands, scratch=(), flops=10**6):
    vmem = pl.BlockSpec(memory_space=pltpu.VMEM)
    return pl.pallas_call(
        kernel,
        out_shape=out_shape,
        in_specs=[vmem] * len(operands),
        out_specs=jax.tree.map(lambda _: vmem, out_shape),
        scratch_shapes=list(scratch),
        compiler_params=pltpu.CompilerParams(vmem_limit_bytes=16 * 2**20),
        cost_estimate=pl.CostEstimate(flops=flops, bytes_accessed=10**7, transcendentals=0),
    )(*operands)


def per_device(sensitivity, precision, reaction, load):
    rows, params = load.shape
    _, columns = reaction.shape
    obs = sensitivity.shape[1]
    plane = lax.axis_size(PLANE)
    line = lax.axis_size(LINE)
    groups = rows // BLOCK
    halves = plane // groups
    piece = obs // halves
    flops = 2 * rows * params * obs

    def smoothed(field, low, high, with_bent):
        prior = jax.ShapeDtypeStruct((rows, params), F32)
        bent = jax.ShapeDtypeStruct((BLOCK, LANES), F32)
        shape = (prior, bent) if with_bent else (prior,)
        return called(prior_kernel, shape, (field, low, high, low_line, high_line, reaction))

    def exchanged(tiles, axis):
        return lax.all_to_all(tiles, axis, 0, 0, tiled=True)

    def observed(operands, width):
        return called(
            functools.partial(forward_kernel, width > piece),
            jax.ShapeDtypeStruct((plane, BLOCK, width), BF16),
            operands,
            [pltpu.VMEM((rows, obs), F32)],
            flops,
        )

    def middle(tiles, *more):
        shape = jax.ShapeDtypeStruct((line, BLOCK, tiles.shape[2]), BF16)
        return called(functools.partial(middle_kernel, piece), shape, (tiles, *more))

    def raised(tiles):
        shape = jax.ShapeDtypeStruct((plane, BLOCK, tiles.shape[2]), BF16)
        return called(functools.partial(raised_kernel, piece), shape, (tiles, precision))

    def projected(tiles, prior):
        return called(
            functools.partial(back_kernel, piece),
            jax.ShapeDtypeStruct((rows, params + tiles.shape[2] - piece), F32),
            (tiles, sensitivity, prior),
            [pltpu.VMEM((LANES, obs), F32), pltpu.VMEM((obs, LANES), BF16)],
            flops,
        )

    edge = 2 * columns

    def with_reaction(part, own):
        return jnp.concatenate([part, jnp.pad(own, ((0, BLOCK - 1), (0, columns)))], axis=0)

    tiles = jnp.dot(load.astype(BF16), sensitivity, preferred_element_type=F32).astype(BF16)
    tiles = tiles.reshape(groups, BLOCK, halves, piece).swapaxes(1, 2).reshape(plane, BLOCK, piece)
    tiles, load, reaction = lax.optimization_barrier((tiles, load, reaction))
    low = passed(with_reaction(load[:, params - edge :], reaction[-1:]), links(1, 1))
    high = passed(with_reaction(load[:, :edge], reaction[:1]), links(1, -1))
    tiles = called(relay_kernel, jax.ShapeDtypeStruct(tiles.shape, BF16), (tiles,))
    tiles = exchanged(tiles, PLANE)
    tiles = middle(tiles)
    tiles, low, high = lax.optimization_barrier((tiles, low, high))
    low_line, high_line = (e[rows : rows + 1, :columns] for e in (low, high))
    (prior,) = smoothed(load, low, high, False)
    tiles, prior, low_line, high_line = lax.optimization_barrier((tiles, prior, low_line, high_line))
    arrived = exchanged(tiles, LINE)
    received = exchanged(raised(arrived), PLANE)
    half = projected(received, prior)
    image = half + lax.ppermute(half, "rhs", SWAP)

    low = passed(image[:, params - edge :], links(1, 1))
    high = passed(image[:, :edge], links(1, -1))
    tiles = observed((image, load, sensitivity), piece + LANES)
    arrived = exchanged(tiles, PLANE)
    shape = jax.ShapeDtypeStruct((1, *arrived.shape[1:]), F32)
    arrived = called(gather_kernel, shape, (arrived,))
    arrived, low, high = lax.optimization_barrier((arrived, low, high))
    prior, bent = smoothed(image, low, high, True)
    tiles, prior = lax.optimization_barrier((middle(arrived, bent), prior))
    arrived = exchanged(tiles, LINE)
    received = exchanged(raised(arrived), PLANE)
    half = projected(received, prior)
    other = lax.ppermute(half, "rhs", SWAP)
    bb, bq, qq, data, bent = (half[:, params + i] for i in range(5))
    qw = data + other[:, params + DATA] + (bent + other[:, params + BENT])

    alpha = bb / bq
    fresh = bb - 2.0 * alpha * bq + alpha * alpha * qq
    beta = fresh / bb
    grown = 1.0 + beta
    curved = grown * grown * bq - 2.0 * alpha * grown * qq + alpha * alpha * qw
    second = fresh / curved
    near = (alpha + second * grown)[:, None]
    far = (alpha * second)[:, None]

    twice = half[:, :params] + other[:, :params]
    solution = near * load - far * image
    residual = load - near * image + far * twice
    return (solution, residual)


def solution(mesh):
    torus = Mesh(
        mesh.devices.reshape(4, 4, 8, mesh.shape["rhs"]), ("tile_0", "tile_1", "tile_2", "rhs")
    )
    placed = (P(TILE, "rhs"), P("rhs"), P(TILE, None), P(None, TILE))

    return jax.shard_map(
        per_device,
        mesh=torus,
        in_specs=placed,
        out_specs=(P(None, TILE), P(None, TILE)),
        check_vma=False,
    )
```
